32 devices in a mesh: row: 8 (over z, y), col: 2 (over core), depth: 2 (over x).
Axes of the slice: x: 2, y: 2, z: 4, core: 2. Of those that a mesh axis runs over, the one named last changes fastest.
Arguments:
- student_hidden: bfloat16 [2048, 768], P('row', ('depth', 'col')), may hold values from -16 to 16
- embedding: bfloat16 [50304, 768], P('col', ('depth', 'row')), as said below
- teacher_logits: bfloat16 [2048, 50304], P('row', ('col', 'depth')), may hold values from -24 to 124, as said below
Outputs:
- loss: float32 [2048], P('row')
- peak_logprob: float32 [2048], P('row')
The draws below stay inside these ranges and needn't reach their ends.
Inputs may be any that keep to these rules, and one draw needn't show every extreme that they name: embedding entries lie within plus or minus 4 / sqrt(768). teacher_logits lie within -24 and 124; each token's logits carry an offset of 0 to 100.
All inputs are finite; a program needn't handle non-finite values.
Results may differ from the reference program's by a relative error of at most 0.0003.
Values may be sent and summed in bfloat16 or wider, within the bound.
A program may use at most 128 MiB of HBM per device.

```python
import jax
import jax.numpy as jnp
from jax import lax

D = 768
VOCAB = 50304
TOK_DEV = 256
TOKENS = 2048
N_ROW = 8


def embedding_table(key):
    base = jax.random.normal(jax.random.fold_in(key, 101), (VOCAB, D), jnp.float32)
    return jnp.clip(base, -4.0, 4.0) * D ** (-0.5)


def draw_embedding(key, part):
    return embedding_table(key).astype(jnp.bfloat16)


def draw_student_hidden(key, part):
    hidden = jnp.clip(jax.random.normal(jax.random.fold_in(key, 205), (TOKENS, D), jnp.float32), -6.0, 6.0)
    return jnp.clip(hidden, -16.0, 16.0).astype(jnp.bfloat16)


def draw_teacher_logits(key, part):
    offsets = jax.random.uniform(jax.random.fold_in(key, 301), (TOKENS, 1), jnp.float32, 0.0, 100.0)
    noise = 4.0 * jnp.clip(jax.random.normal(jax.random.fold_in(key, 304), (TOKENS, VOCAB), jnp.float32), -6.0, 6.0)
    return (offsets + noise).astype(jnp.bfloat16)


def setup_inputs(seed: int = 0) -> dict:
    streams_of = jax.random.split(jax.random.key(seed), 4)
    student_hidden = draw_student_hidden(jax.random.fold_in(streams_of[3], 71), 0)
    embedding = draw_embedding(jax.random.fold_in(streams_of[3], 71), 0)
    teacher_logits = draw_teacher_logits(jax.random.fold_in(streams_of[3], 71), 0)
    return {"student_hidden": student_hidden, "embedding": embedding, "teacher_logits": teacher_logits}


def reference(student_hidden, embedding, teacher_logits):
    def token_block(pair):
        hidden_rows, teacher_rows = pair
        student = jnp.dot(hidden_rows, embedding.T, preferred_element_type=jnp.float32)
        teacher_values = teacher_rows.astype(jnp.float32)
        student_peak = jnp.max(student, axis=1)
        teacher_peak = jnp.max(teacher_values, axis=1)
        student_sum = jnp.sum(jnp.exp(student - student_peak[:, None]), axis=1)
        weights = jnp.exp(teacher_values - teacher_peak[:, None])
        teacher_sum = jnp.sum(weights, axis=1)
        cross_sum = jnp.sum(weights * student, axis=1)
        norm_log = jnp.log(student_sum)
        return student_peak + norm_log - cross_sum / teacher_sum, -norm_log

    losses, peaks = lax.map(token_block, (student_hidden.reshape(N_ROW, TOK_DEV, D), teacher_logits.reshape(N_ROW, TOK_DEV, VOCAB)))
    return losses.reshape(TOKENS), peaks.reshape(TOKENS)
```

```python
import functools

import jax
import jax.numpy as jnp
from jax import lax
from jax.experimental import pallas as pl
from jax.experimental.pallas import tpu as pltpu
from jax.sharding import PartitionSpec as P

MESH = pl.DeviceIdType.MESH
GROUP = 2
TILE = 640
LOW = -1e30


def place(rows, cols, depths):
    r, c, d = lax.axis_index("row"), lax.axis_index("col"), lax.axis_index("depth")
    return r, c, d, r // GROUP, lax.rem(r, GROUP)


def greet(targets):
    barrier = pltpu.get_barrier_semaphore()
    for row, col, depth in targets:
        pl.semaphore_signal(barrier, inc=1, device_id=(row, col, depth), device_id_type=MESH)
    return barrier


def group_peers(rows, cols, depths):
    r, c, d, q, j = place(rows, cols, depths)
    peers = []
    for dj in range(GROUP):
        for dc in range(cols):
            for dd in range(depths):
                if dj or dc or dd:
                    peers.append((q * GROUP + lax.rem(j + dj, GROUP), lax.rem(c + dc, cols), lax.rem(d + dd, depths), dj))
    return peers


def gather_kernel(
    rows, cols, depths, pieces_ref, teacher_ref, hidden_ref, full_ref, other_ref, hid_ref,
    own_sem, first_send, first_recv, right_send, left_send, line_recv, teach_send, teach_recv, hid_send, hid_recv,
):
    r, c, d, q, j = place(rows, cols, depths)
    steps = rows // GROUP
    count = depths * GROUP
    me = d * GROUP + j
    peers = group_peers(rows, cols, depths)

    def slot(block, piece):
        return (piece // GROUP) * rows + block * GROUP + lax.rem(piece, GROUP)

    barrier = greet([(a, b, e) for a, b, e, _ in peers])

    @pl.when(q + 1 < steps)
    def _():
        pl.semaphore_signal(barrier, inc=1, device_id=(r + GROUP, c, d), device_id_type=MESH)

    @pl.when(q > 0)
    def _():
        pl.semaphore_signal(barrier, inc=1, device_id=(r - GROUP, c, d), device_id_type=MESH)

    neighbours = (q + 1 < steps).astype(jnp.int32) + (q > 0).astype(jnp.int32)
    pl.semaphore_wait(barrier, len(peers) + neighbours)

    def first(off):
        target = lax.rem(me + off, count)
        return pltpu.make_async_remote_copy(
            src_ref=pieces_ref.at[target], dst_ref=full_ref.at[slot(q, me)],
            send_sem=first_send.at[off], recv_sem=first_recv.at[off],
            device_id=(q * GROUP + lax.rem(target, GROUP), c, target // GROUP), device_id_type=MESH,
        )

    def along(block, off, right, src=None):
        piece = lax.rem(me + count - off, count)
        at = slot(block, piece)
        sems = right_send if right else left_send
        return pltpu.make_async_remote_copy(
            src_ref=full_ref.at[at] if src is None else src, dst_ref=full_ref.at[at],
            send_sem=sems.at[block, off], recv_sem=line_recv.at[block, off],
            device_id=(r + GROUP if right else r - GROUP, c, d), device_id_type=MESH,
        )

    def both(block, off, src=None):
        @pl.when(q + 1 < steps)
        def _():
            along(block, off, True, src).start()

        @pl.when(q > 0)
        def _():
            along(block, off, False, src).start()

    both(q, 0, pieces_ref.at[me])
    firsts = [first(off) for off in range(1, count)]
    for copy in firsts:
        copy.start()
    hids = []
    for n, (a, b, e, dj) in enumerate(peers):
        hids.append(pltpu.make_async_remote_copy(
            src_ref=hidden_ref, dst_ref=hid_ref.at[dj, d * cols + c], send_sem=hid_send.at[n], recv_sem=hid_recv.at[n],
            device_id=(a, b, e), device_id_type=MESH,
        ))
        hids[-1].start()
    pj = lax.rem(j + 1, GROUP)
    teach = pltpu.make_async_remote_copy(
        src_ref=teacher_ref.at[pj], dst_ref=other_ref, send_sem=teach_send, recv_sem=teach_recv,
        device_id=(q * GROUP + pj, c, d), device_id_type=MESH,
    )
    teach.start()
    own = pltpu.make_async_copy(pieces_ref.at[me], full_ref.at[slot(q, me)], own_sem.at[0])
    own.start()
    own_hid = pltpu.make_async_copy(hidden_ref, hid_ref.at[0, d * cols + c], own_sem.at[1])
    own_hid.start()

    for off in range(1, count):
        firsts[off - 1].wait_recv()
        both(q, off)

    def step(k, _):
        for off in range(count):
            @pl.when(q - k >= 0)
            def _():
                along(q - k, off, True).wait_recv()

                @pl.when(q + 1 < steps)
                def _():
                    along(q - k, off, True).start()

            @pl.when(q + k < steps)
            def _():
                along(q + k, off, False).wait_recv()

                @pl.when(q > 0)
                def _():
                    along(q + k, off, False).start()

        return 0

    lax.fori_loop(1, steps, step, 0)

    def settle(block, _):
        for off in range(count):
            @pl.when((block <= q) & (q + 1 < steps))
            def _():
                along(block, off, True).wait_send()

            @pl.when((block >= q) & (q > 0))
            def _():
                along(block, off, False).wait_send()

        return 0

    lax.fori_loop(0, steps, settle, 0)
    for copy in firsts:
        copy.wait_send()
    for copy in hids:
        copy.wait()
    teach.wait()
    own.wait()
    own_hid.wait()


def gather(rows, cols, depths, pieces, teacher, hidden):
    count, narrow, width = pieces.shape
    steps = rows // GROUP
    features, tokens = hidden.shape
    peers = GROUP * cols * depths - 1
    dma = pltpu.SemaphoreType.DMA
    any_space = pl.BlockSpec(memory_space=pl.ANY)
    return pl.pallas_call(
        functools.partial(gather_kernel, rows, cols, depths),
        out_shape=(
            jax.ShapeDtypeStruct((depths * rows, narrow, width), pieces.dtype),
            jax.ShapeDtypeStruct((width, tokens), teacher.dtype),
            jax.ShapeDtypeStruct((GROUP, depths * cols, features, tokens), hidden.dtype),
        ),
        in_specs=[any_space] * 3,
        out_specs=[any_space] * 3,
        scratch_shapes=[
            dma((2,)), dma((count,)), dma((count,)), dma((steps, count)), dma((steps, count)), dma((steps, count)),
            dma, dma, dma((peers,)), dma((peers,)),
        ],
        compiler_params=pltpu.CompilerParams(collective_id=0, has_side_effects=True),
        name="gather",
    )(pieces, teacher, hidden)


def add_terms(full_ref, teacher_refs, hid_ref, acc, start, size):
    rows = full_ref[:, :, pl.ds(start, size)].reshape(-1, size)
    for n, teacher_ref in enumerate(teacher_refs):
        hidden = hid_ref[n].reshape(rows.shape[0], -1)
        tokens = hidden.shape[1]
        student = lax.dot_general(rows, hidden, (((0,), (0,)), ((), ())), preferred_element_type=jnp.float32)
        student = student.reshape(size // 8, 8, tokens)
        teacher = teacher_ref[pl.ds(start, size), :].astype(jnp.float32).reshape(size // 8, 8, tokens)
        top = jnp.maximum(acc[n, 0], jnp.max(student, axis=0))
        acc[n, 1] = acc[n, 1] * jnp.exp(acc[n, 0] - top) + jnp.sum(jnp.exp(student - top[None]), axis=0)
        acc[n, 0] = top
        teacher_top = jnp.maximum(acc[n, 2], jnp.max(teacher, axis=0))
        fade = jnp.exp(acc[n, 2] - teacher_top)
        weights = jnp.exp(teacher - teacher_top[None])
        acc[n, 3] = acc[n, 3] * fade + jnp.sum(weights, axis=0)
        acc[n, 4] = acc[n, 4] * fade + jnp.sum(weights * student, axis=0)
        acc[n, 2] = teacher_top


def all_terms(full_ref, teacher_refs, hid_ref, out_ref, acc):
    width = full_ref.shape[2]
    for n in range(GROUP):
        for k in range(5):
            acc[n, k] = jnp.full(acc.shape[2:], LOW if k in (0, 2) else 0.0, jnp.float32)

    def tile(i, _):
        add_terms(full_ref, teacher_refs, hid_ref, acc, pl.multiple_of(i * TILE, TILE), TILE)
        return 0

    lax.fori_loop(0, width // TILE, tile, 0)
    if width % TILE:
        add_terms(full_ref, teacher_refs, hid_ref, acc, width - width % TILE, width % TILE)
    for n in range(GROUP):
        values = merge([acc[n, k] for k in range(5)])
        out_ref[n] = jnp.concatenate(values + [values[0]] * 3, axis=0)


def terms_kernel(j_ref, full_ref, own_ref, other_ref, hid_ref, out_ref, acc):
    all_terms(full_ref, (own_ref.at[0], other_ref), hid_ref, out_ref, acc)


def merge(parts):
    top, total, teacher_top, teacher_total, cross = parts
    peak = jnp.max(top, axis=0, keepdims=True)
    teacher_peak = jnp.max(teacher_top, axis=0, keepdims=True)
    scale = jnp.exp(teacher_top - teacher_peak)
    return [
        peak,
        jnp.sum(total * jnp.exp(top - peak), axis=0, keepdims=True),
        teacher_peak,
        jnp.sum(teacher_total * scale, axis=0, keepdims=True),
        jnp.sum(cross * scale, axis=0, keepdims=True),
    ]


def terms(j, full, teacher, other, hid):
    tokens = other.shape[1]
    return pl.pallas_call(
        terms_kernel,
        out_shape=jax.ShapeDtypeStruct((GROUP, 8, tokens), jnp.float32),
        grid_spec=pltpu.PrefetchScalarGridSpec(
            num_scalar_prefetch=1,
            grid=(1,),
            in_specs=[
                pl.BlockSpec(full.shape, lambda i, j: (0, 0, 0)),
                pl.BlockSpec((1,) + other.shape, lambda i, j: (j[0], 0, 0)),
                pl.BlockSpec(other.shape, lambda i, j: (0, 0)),
                pl.BlockSpec(hid.shape, lambda i, j: (0, 0, 0, 0)),
            ],
            out_specs=pl.BlockSpec((GROUP, 8, tokens), lambda i, j: (0, 0, 0)),
            scratch_shapes=[pltpu.VMEM((GROUP, 5, 8, tokens), jnp.float32)],
        ),
        compiler_params=pltpu.CompilerParams(vmem_limit_bytes=60 * 2**20),
        name="terms",
    )(j, full, teacher, other, hid)


def combine_kernel(rows, cols, depths, stats_ref, loss_ref, peak_ref, held, send_sem, recv_sem):
    peers = group_peers(rows, cols, depths)
    barrier = greet([(a, b, e) for a, b, e, _ in peers])
    pl.semaphore_wait(barrier, len(peers))
    copies = []
    for n, (a, b, e, dj) in enumerate(peers):
        copies.append(pltpu.make_async_remote_copy(
            src_ref=stats_ref.at[dj], dst_ref=held.at[n], send_sem=send_sem.at[n], recv_sem=recv_sem.at[n],
            device_id=(a, b, e), device_id_type=MESH,
        ))
        copies[-1].start()
    for copy in copies:
        copy.wait()
    blocks = [stats_ref[0]] + [held[n] for n in range(len(peers))]
    parts = [jnp.concatenate([block[k : k + 1] for block in blocks], axis=0) for k in range(5)]
    peak, total, _, teacher_total, cross = merge(parts)
    norm_log = jnp.log(total)
    loss_ref[...] = peak + norm_log - cross / teacher_total
    peak_ref[...] = -norm_log


def combine(rows, cols, depths, stats):
    tokens = stats.shape[2]
    peers = GROUP * cols * depths - 1
    vmem = pl.BlockSpec(memory_space=pltpu.VMEM)
    return pl.pallas_call(
        functools.partial(combine_kernel, rows, cols, depths),
        out_shape=(jax.ShapeDtypeStruct((1, tokens), jnp.float32),) * 2,
        in_specs=[vmem],
        out_specs=(vmem, vmem),
        scratch_shapes=[
            pltpu.VMEM((peers, 8, tokens), jnp.float32),
            pltpu.SemaphoreType.DMA((peers,)),
            pltpu.SemaphoreType.DMA((peers,)),
        ],
        compiler_params=pltpu.CompilerParams(collective_id=1, has_side_effects=True),
        name="combine",
    )(stats)


def on_device(rows, cols, depths, student_hidden, embedding, teacher_logits):
    vocab, narrow = embedding.shape
    width = vocab // (depths * GROUP)
    pieces = embedding.T.reshape(narrow, depths * GROUP, width).transpose(1, 0, 2)
    teacher = teacher_logits.T.reshape(GROUP, width, -1)
    full, other, hid = gather(rows, cols, depths, pieces, teacher, student_hidden.T)
    j = lax.rem(lax.axis_index("row"), GROUP).astype(jnp.int32).reshape(1)
    loss, peak = combine(rows, cols, depths, terms(j, full, teacher, other, hid))
    return loss.reshape(-1), peak.reshape(-1)


def solution(mesh):
    sizes = [mesh.shape[name] for name in ("row", "col", "depth")]
    in_specs = (P("row", ("depth", "col")), P("col", ("depth", "row")), P("row", ("col", "depth")))
    out_specs = (P("row"), P("row"))
    return jax.shard_map(
        functools.partial(on_device, *sizes), mesh=mesh, in_specs=in_specs, out_specs=out_specs, check_vma=False
    )
```

```python
import functools

import jax
import jax.numpy as jnp
from jax import lax
from jax.experimental import pallas as pl
from jax.experimental.pallas import tpu as pltpu
from jax.sharding import PartitionSpec as P

MESH = pl.DeviceIdType.MESH
GROUP = 2
TILE = 640
CHUNK = 1280
SKIP = 2
LOW = -1e30


def place(rows, cols, depths):
    r, c, d = lax.axis_index("row"), lax.axis_index("col"), lax.axis_index("depth")
    return r, c, d, r // GROUP, lax.rem(r, GROUP)


def greet(targets):
    barrier = pltpu.get_barrier_semaphore()
    for row, col, depth in targets:
        pl.semaphore_signal(barrier, inc=1, device_id=(row, col, depth), device_id_type=MESH)
    return barrier


def group_peers(rows, cols, depths):
    r, c, d, q, j = place(rows, cols, depths)
    peers = []
    for dj in range(GROUP):
        for dc in range(cols):
            for dd in range(depths):
                if dj or dc or dd:
                    peers.append((q * GROUP + lax.rem(j + dj, GROUP), lax.rem(c + dc, cols), lax.rem(d + dd, depths), dj))
    return peers


def ends(rows, q):
    steps = rows // GROUP
    low, high = q == 0, q == steps - 1
    return low | high, (q == 1) | (q == steps - 2), jnp.where(q * 2 < steps, GROUP, -GROUP)


def as_count(flag):
    return flag.astype(jnp.int32)


def gather_kernel(
    rows, cols, depths, pieces_ref, teacher_ref, hidden_ref, full_ref, other_ref, extra_ref, hid_ref,
    own_sem, first_send, first_recv, right_send, left_send, line_recv, teach_send, teach_recv, extra_send, extra_recv,
    hid_send, hid_recv, far_send, far_recv,
):
    r, c, d, q, j = place(rows, cols, depths)
    steps = rows // GROUP
    count = depths * GROUP
    chunks = full_ref.shape[2] // CHUNK
    kept = chunks - SKIP
    me = d * GROUP + j
    peers = group_peers(rows, cols, depths)
    end, server, inward = ends(rows, q)

    def slot(block, piece):
        return (piece // GROUP) * rows + block * GROUP + lax.rem(piece, GROUP)

    def lanes(t):
        return pl.ds(pl.multiple_of(t * CHUNK, CHUNK), CHUNK)

    barrier = greet([(a, b, e) for a, b, e, _ in peers])

    @pl.when(q + 1 < steps)
    def _():
        pl.semaphore_signal(barrier, inc=1, device_id=(r + GROUP, c, d), device_id_type=MESH)

    @pl.when(q > 0)
    def _():
        pl.semaphore_signal(barrier, inc=1, device_id=(r - GROUP, c, d), device_id_type=MESH)

    pl.semaphore_wait(barrier, len(peers) + as_count(q + 1 < steps) + as_count(q > 0))

    def first(t, off):
        target = lax.rem(me + off, count)
        return pltpu.make_async_remote_copy(
            src_ref=pieces_ref.at[target, :, lanes(t)], dst_ref=full_ref.at[slot(q, me), :, lanes(t)],
            send_sem=first_send.at[t, off], recv_sem=first_recv.at[t, off],
            device_id=(q * GROUP + lax.rem(target, GROUP), c, target // GROUP), device_id_type=MESH,
        )

    def along(block, t, off, right, own=False):
        piece = lax.rem(me + count - off, count)
        at = full_ref.at[slot(block, piece), :, lanes(t)]
        sems = right_send if right else left_send
        return pltpu.make_async_remote_copy(
            src_ref=pieces_ref.at[me, :, lanes(t)] if own else at, dst_ref=at,
            send_sem=sems.at[block, t, off], recv_sem=line_recv.at[block, t, off],
            device_id=(r + GROUP if right else r - GROUP, c, d), device_id_type=MESH,
        )

    def to_right(t):
        return (q + 1 < steps) & ((t < kept) | (q + 2 < steps))

    def to_left(t):
        return (q > 0) & ((t < kept) | (q > 1))

    def both(t, off, own=False):
        @pl.when(to_right(t))
        def _():
            along(q, t, off, True, own).start()

        @pl.when(to_left(t))
        def _():
            along(q, t, off, False, own).start()

    def launch(t, _):
        for off in range(1, count):
            first(t, off).start()
        return 0

    both(0, 0, True)
    lax.fori_loop(0, chunks, launch, 0)
    hids = []
    for n, (a, b, e, dj) in enumerate(peers):
        hids.append(pltpu.make_async_remote_copy(
            src_ref=hidden_ref, dst_ref=hid_ref.at[dj, d * cols + c], send_sem=hid_send.at[n], recv_sem=hid_recv.at[n],
            device_id=(a, b, e), device_id_type=MESH,
        ))
        hids[-1].start()
    pj = lax.rem(j + 1, GROUP)
    cut = kept * CHUNK
    tail = pl.ds(cut, other_ref.shape[0] - cut)

    def teach(n, part):
        return pltpu.make_async_remote_copy(
            src_ref=teacher_ref.at[pj, part], dst_ref=other_ref.at[part], send_sem=teach_send.at[n], recv_sem=teach_recv.at[n],
            device_id=(q * GROUP + pj, c, d), device_id_type=MESH,
        )

    teaches = [teach(0, tail), teach(1, pl.ds(0, cut))]
    for copy in teaches:
        copy.start()

    def extra(n):
        return pltpu.make_async_remote_copy(
            src_ref=teacher_ref.at[j, tail] if n == 0 else other_ref.at[tail], dst_ref=extra_ref.at[n],
            send_sem=extra_send.at[n], recv_sem=extra_recv.at[n], device_id=(r + inward, c, d), device_id_type=MESH,
        )

    far = [pltpu.make_async_remote_copy(
        src_ref=hidden_ref, dst_ref=hid_ref.at[GROUP, d * cols + c], send_sem=far_send.at[0], recv_sem=far_recv.at[0],
        device_id=(r + inward, c, d), device_id_type=MESH,
    )]
    for n, (a, b, e, dj) in enumerate(peers):
        far.append(pltpu.make_async_remote_copy(
            src_ref=hid_ref.at[GROUP, d * cols + c], dst_ref=hid_ref.at[GROUP + dj, d * cols + c],
            send_sem=far_send.at[n + 1], recv_sem=far_recv.at[n + 1], device_id=(a, b, e), device_id_type=MESH,
        ))

    @pl.when(end)
    def _():
        far[0].start()

    own = pltpu.make_async_copy(pieces_ref.at[me], full_ref.at[slot(q, me)], own_sem.at[0])
    own.start()
    own_hid = pltpu.make_async_copy(hidden_ref, hid_ref.at[0, d * cols + c], own_sem.at[1])
    own_hid.start()

    def start_line(t, _):
        @pl.when(t > 0)
        def _():
            both(t, 0, True)

        for off in range(1, count):
            first(t, off).wait_recv()
            both(t, off)
        return 0

    lax.fori_loop(0, chunks, start_line, 0)

    @pl.when(end)
    def _():
        extra(0).start()
        teaches[0].wait_recv()
        extra(1).start()

    @pl.when(server)
    def _():
        far[0].wait_recv()
        for copy in far[1:]:
            copy.start()

    def step(k, _):
        def chunk(t, _):
            wanted = (t < kept) | ~end
            for off in range(count):
                @pl.when((q - k >= 0) & wanted)
                def _():
                    along(q - k, t, off, True).wait_recv()

                    @pl.when(to_right(t))
                    def _():
                        along(q - k, t, off, True).start()

                @pl.when((q + k < steps) & wanted)
                def _():
                    along(q + k, t, off, False).wait_recv()

                    @pl.when(to_left(t))
                    def _():
                        along(q + k, t, off, False).start()

            return 0

        return lax.fori_loop(0, chunks, chunk, 0)

    lax.fori_loop(1, steps, step, 0)

    def settle(block, _):
        def chunk(t, _):
            for off in range(count):
                @pl.when((block <= q) & to_right(t))
                def _():
                    along(block, t, off, True).wait_send()

                @pl.when((block >= q) & to_left(t))
                def _():
                    along(block, t, off, False).wait_send()

            return 0

        return lax.fori_loop(0, chunks, chunk, 0)

    lax.fori_loop(0, steps, settle, 0)

    def settle_first(t, _):
        for off in range(1, count):
            first(t, off).wait_send()
        return 0

    lax.fori_loop(0, chunks, settle_first, 0)
    for copy in hids:
        copy.wait()
    teaches[1].wait()
    teaches[0].wait_send()
    own.wait()
    own_hid.wait()

    @pl.when(end)
    def _():
        far[0].wait_send()
        extra(0).wait_send()
        extra(1).wait_send()

    @pl.when(~end)
    def _():
        teaches[0].wait_recv()

    @pl.when(server)
    def _():
        extra(0).wait_recv()
        extra(1).wait_recv()
        for copy in far[1:]:
            copy.wait()


def gather(rows, cols, depths, pieces, teacher, hidden):
    count, narrow, padded = pieces.shape
    width = teacher.shape[1]
    steps = rows // GROUP
    chunks = padded // CHUNK
    features, tokens = hidden.shape
    peers = GROUP * cols * depths - 1
    dma = pltpu.SemaphoreType.DMA
    any_space = pl.BlockSpec(memory_space=pl.ANY)
    line = (steps, chunks, count)
    return pl.pallas_call(
        functools.partial(gather_kernel, rows, cols, depths),
        out_shape=(
            jax.ShapeDtypeStruct((depths * rows, narrow, padded), pieces.dtype),
            jax.ShapeDtypeStruct((width, tokens), teacher.dtype),
            jax.ShapeDtypeStruct((GROUP, width - (chunks - SKIP) * CHUNK, tokens), teacher.dtype),
            jax.ShapeDtypeStruct((2 * GROUP, depths * cols, features, tokens), hidden.dtype),
        ),
        in_specs=[any_space] * 3,
        out_specs=[any_space] * 4,
        scratch_shapes=[
            dma((2,)), dma((chunks, count)), dma((chunks, count)), dma(line), dma(line), dma(line),
            dma((2,)), dma((2,)), dma((2,)), dma((2,)), dma((peers,)), dma((peers,)), dma((peers + 1,)), dma((peers + 1,)),
        ],
        compiler_params=pltpu.CompilerParams(collective_id=0, has_side_effects=True),
        name="gather",
    )(pieces, teacher, hidden)


def add_terms(full_ref, teacher_refs, hid_ref, acc, start, size, offset=0, sets=range(GROUP)):
    rows = full_ref[:, :, pl.ds(start, size)].reshape(-1, size)
    for n, teacher_ref in zip(sets, teacher_refs):
        hidden = hid_ref[n].reshape(rows.shape[0], -1)
        tokens = hidden.shape[1]
        student = lax.dot_general(rows, hidden, (((0,), (0,)), ((), ())), preferred_element_type=jnp.float32)
        student = student.reshape(size // 8, 8, tokens)
        teacher = teacher_ref[pl.ds(start - offset, size), :].astype(jnp.float32).reshape(size // 8, 8, tokens)
        top = jnp.maximum(acc[n, 0], jnp.max(student, axis=0))
        acc[n, 1] = acc[n, 1] * jnp.exp(acc[n, 0] - top) + jnp.sum(jnp.exp(student - top[None]), axis=0)
        acc[n, 0] = top
        teacher_top = jnp.maximum(acc[n, 2], jnp.max(teacher, axis=0))
        fade = jnp.exp(acc[n, 2] - teacher_top)
        weights = jnp.exp(teacher - teacher_top[None])
        acc[n, 3] = acc[n, 3] * fade + jnp.sum(weights, axis=0)
        acc[n, 4] = acc[n, 4] * fade + jnp.sum(weights * student, axis=0)
        acc[n, 2] = teacher_top


def terms_kernel(flags, full_ref, own_ref, other_ref, extra_ref, hid_ref, out_ref, acc):
    width = other_ref.shape[0]
    cut = width - extra_ref.shape[1]
    for n in range(2 * GROUP):
        for k in range(5):
            acc[n, k] = jnp.full(acc.shape[2:], LOW if k in (0, 2) else 0.0, jnp.float32)
    main = (own_ref.at[0], other_ref)
    extra = tuple(extra_ref.at[n] for n in range(GROUP))

    def tiles(begin, stop, refs, offset, sets):
        whole = (stop - begin) // TILE

        def tile(i, _):
            start = pl.multiple_of(begin + i * TILE, 128)
            add_terms(full_ref, refs, hid_ref, acc, start, TILE, offset, sets)
            return 0

        lax.fori_loop(0, whole, tile, 0)
        if (stop - begin) % TILE:
            add_terms(full_ref, refs, hid_ref, acc, begin + whole * TILE, (stop - begin) % TILE, offset, sets)

    tiles(0, cut, main, 0, range(GROUP))

    @pl.when(flags[1] == 0)
    def _():
        tiles(cut, width, main, 0, range(GROUP))

    @pl.when(flags[2] == 1)
    def _():
        tiles(cut, width, extra, cut, range(GROUP, 2 * GROUP))

    for n in range(2 * GROUP):
        values = merge([acc[n, k] for k in range(5)])
        out_ref[n] = jnp.concatenate(values + [values[0]] * 3, axis=0)


def merge(parts):
    top, total, teacher_top, teacher_total, cross = parts
    peak = jnp.max(top, axis=0, keepdims=True)
    teacher_peak = jnp.max(teacher_top, axis=0, keepdims=True)
    scale = jnp.exp(teacher_top - teacher_peak)
    return [
        peak,
        jnp.sum(total * jnp.exp(top - peak), axis=0, keepdims=True),
        teacher_peak,
        jnp.sum(teacher_total * scale, axis=0, keepdims=True),
        jnp.sum(cross * scale, axis=0, keepdims=True),
    ]


def terms(flags, full, teacher, other, extra, hid):
    tokens = other.shape[1]
    return pl.pallas_call(
        terms_kernel,
        out_shape=jax.ShapeDtypeStruct((2 * GROUP, 8, tokens), jnp.float32),
        grid_spec=pltpu.PrefetchScalarGridSpec(
            num_scalar_prefetch=1,
            grid=(1,),
            in_specs=[
                pl.BlockSpec(full.shape, lambda i, f: (0, 0, 0)),
                pl.BlockSpec((1,) + other.shape, lambda i, f: (f[0], 0, 0)),
                pl.BlockSpec(other.shape, lambda i, f: (0, 0)),
                pl.BlockSpec(extra.shape, lambda i, f: (0, 0, 0)),
                pl.BlockSpec(hid.shape, lambda i, f: (0, 0, 0, 0)),
            ],
            out_specs=pl.BlockSpec((2 * GROUP, 8, tokens), lambda i, f: (0, 0, 0)),
            scratch_shapes=[pltpu.VMEM((2 * GROUP, 5, 8, tokens), jnp.float32)],
        ),
        compiler_params=pltpu.CompilerParams(vmem_limit_bytes=60 * 2**20),
        name="terms",
    )(flags, full, teacher, other, extra, hid)


def combine_kernel(rows, cols, depths, stats_ref, loss_ref, peak_ref, held, send_sem, recv_sem):
    r, c, d, q, j = place(rows, cols, depths)
    end, server, inward = ends(rows, q)
    peers = group_peers(rows, cols, depths)
    near = len(peers)
    group = [(r, c, d, 0)] + peers
    barrier = greet([(a, b, e) for a, b, e, _ in peers])

    @pl.when(end)
    def _():
        greet([(a + inward, b, e) for a, b, e, _ in group])

    @pl.when(server)
    def _():
        greet([(a - inward, b, e) for a, b, e, _ in group])

    pl.semaphore_wait(barrier, near + as_count(end | server) * len(group))

    def send(n, a, b, e, source):
        return pltpu.make_async_remote_copy(
            src_ref=stats_ref.at[source], dst_ref=held.at[n], send_sem=send_sem.at[n], recv_sem=recv_sem.at[n],
            device_id=(a, b, e), device_id_type=MESH,
        )

    copies = [send(n, a, b, e, dj) for n, (a, b, e, dj) in enumerate(peers)]
    far = [send(near + n, a - inward, b, e, GROUP + dj) for n, (a, b, e, dj) in enumerate(group)]

    @pl.when(server)
    def _():
        for copy in far:
            copy.start()

    for copy in copies:
        copy.start()

    @pl.when(~end)
    def _():
        for n in range(len(group)):
            for k in range(5):
                held[near + n, k] = jnp.full(held.shape[2:], LOW if k in (0, 2) else 0.0, jnp.float32)

    for copy in copies:
        copy.wait()

    @pl.when(server)
    def _():
        for copy in far:
            copy.wait_send()

    @pl.when(end)
    def _():
        for copy in far:
            copy.wait_recv()

    blocks = [stats_ref[0]] + [held[n] for n in range(near + len(group))]
    parts = [jnp.concatenate([block[k : k + 1] for block in blocks], axis=0) for k in range(5)]
    peak, total, _, teacher_total, cross = merge(parts)
    norm_log = jnp.log(total)
    loss_ref[...] = peak + norm_log - cross / teacher_total
    peak_ref[...] = -norm_log


def combine(rows, cols, depths, stats):
    tokens = stats.shape[2]
    slots = 2 * GROUP * cols * depths - 1
    vmem = pl.BlockSpec(memory_space=pltpu.VMEM)
    return pl.pallas_call(
        functools.partial(combine_kernel, rows, cols, depths),
        out_shape=(jax.ShapeDtypeStruct((1, tokens), jnp.float32),) * 2,
        in_specs=[vmem],
        out_specs=(vmem, vmem),
        scratch_shapes=[
            pltpu.VMEM((slots, 8, tokens), jnp.float32),
            pltpu.SemaphoreType.DMA((slots,)),
            pltpu.SemaphoreType.DMA((slots,)),
        ],
        compiler_params=pltpu.CompilerParams(collective_id=1, has_side_effects=True),
        name="combine",
    )(stats)


def on_device(rows, cols, depths, student_hidden, embedding, teacher_logits):
    vocab, narrow = embedding.shape
    width = vocab // (depths * GROUP)
    pieces = embedding.T.reshape(narrow, depths * GROUP, width).transpose(1, 0, 2)
    pieces = jnp.pad(pieces, ((0, 0), (0, 0), (0, -width % CHUNK)))
    teacher = teacher_logits.T.reshape(GROUP, width, -1)
    full, other, extra, hid = gather(rows, cols, depths, pieces, teacher, student_hidden.T)
    row = lax.axis_index("row")
    end, server, _ = ends(rows, row // GROUP)
    flags = jnp.stack([lax.rem(row, GROUP), as_count(end), as_count(server)]).astype(jnp.int32)
    loss, peak = combine(rows, cols, depths, terms(flags, full, teacher, other, extra, hid))
    return loss.reshape(-1), peak.reshape(-1)


def solution(mesh):
    sizes = [mesh.shape[name] for name in ("row", "col", "depth")]
    in_specs = (P("row", ("depth", "col")), P("col", ("depth", "row")), P("row", ("col", "depth")))
    out_specs = (P("row"), P("row"))
    return jax.shard_map(
        functools.partial(on_device, *sizes), mesh=mesh, in_specs=in_specs, out_specs=out_specs, check_vma=False
    )
```

```python
import functools

import jax
import jax.numpy as jnp
from jax import lax
from jax.experimental import pallas as pl
from jax.experimental.pallas import tpu as pltpu
from jax.sharding import PartitionSpec as P

MESH = pl.DeviceIdType.MESH
GROUP = 2
TILE = 640
CHUNK = 640
SKIP = 3
LOW = -1e30


def place(rows, cols, depths):
    r, c, d = lax.axis_index("row"), lax.axis_index("col"), lax.axis_index("depth")
    return r, c, d, r // GROUP, lax.rem(r, GROUP)


def greet(targets):
    barrier = pltpu.get_barrier_semaphore()
    for row, col, depth in targets:
        pl.semaphore_signal(barrier, inc=1, device_id=(row, col, depth), device_id_type=MESH)
    return barrier


def group_peers(rows, cols, depths):
    r, c, d, q, j = place(rows, cols, depths)
    peers = []
    for dj in range(GROUP):
        for dc in range(cols):
            for dd in range(depths):
                if dj or dc or dd:
                    peers.append((q * GROUP + lax.rem(j + dj, GROUP), lax.rem(c + dc, cols), lax.rem(d + dd, depths), dj))
    return peers


def ends(rows, q):
    steps = rows // GROUP
    low, high = q == 0, q == steps - 1
    return low | high, (q == 1) | (q == steps - 2), jnp.where(q * 2 < steps, GROUP, -GROUP)


def as_count(flag):
    return flag.astype(jnp.int32)


def gather_kernel(
    rows, cols, depths, pieces_ref, teacher_ref, hidden_ref, full_ref, other_ref, extra_ref, hid_ref,
    own_sem, first_send, first_recv, line_send, line_recv, teach_send, teach_recv, extra_send, extra_recv,
    hid_send, hid_recv, far_send, far_recv,
):
    r, c, d, q, j = place(rows, cols, depths)
    steps = rows // GROUP
    count = depths * GROUP
    chunks = full_ref.shape[2] // CHUNK
    kept = chunks - SKIP
    me = d * GROUP + j
    peers = group_peers(rows, cols, depths)
    end, server, inward = ends(rows, q)

    def slot(block, piece):
        return (piece // GROUP) * rows + block * GROUP + lax.rem(piece, GROUP)

    def lanes(t):
        return pl.ds(pl.multiple_of(t * CHUNK, CHUNK), CHUNK)

    barrier = greet([(a, b, e) for a, b, e, _ in peers])

    @pl.when(q + 1 < steps)
    def _():
        pl.semaphore_signal(barrier, inc=1, device_id=(r + GROUP, c, d), device_id_type=MESH)

    @pl.when(q > 0)
    def _():
        pl.semaphore_signal(barrier, inc=1, device_id=(r - GROUP, c, d), device_id_type=MESH)

    pl.semaphore_wait(barrier, len(peers) + as_count(q + 1 < steps) + as_count(q > 0))

    def first(t, off):
        target = lax.rem(me + off, count)
        return pltpu.make_async_remote_copy(
            src_ref=pieces_ref.at[target, :, lanes(t)], dst_ref=full_ref.at[slot(q, me), :, lanes(t)],
            send_sem=first_send.at[t, off], recv_sem=first_recv.at[t, off],
            device_id=(q * GROUP + lax.rem(target, GROUP), c, target // GROUP), device_id_type=MESH,
        )

    def along(block, t, off, right, own=False):
        piece = lax.rem(me + count - off, count)
        at = full_ref.at[slot(block, piece), :, lanes(t)]
        return pltpu.make_async_remote_copy(
            src_ref=pieces_ref.at[me, :, lanes(t)] if own else at, dst_ref=at,
            send_sem=line_send.at[block if right else block + 1, t, off], recv_sem=line_recv.at[block, t, off],
            device_id=(r + GROUP if right else r - GROUP, c, d), device_id_type=MESH,
        )

    def to_right(t):
        return (q + 1 < steps) & ((t < kept) | (q + 2 < steps))

    def to_left(t):
        return (q > 0) & ((t < kept) | (q > 1))

    def both(t, off, own=False):
        @pl.when(to_right(t))
        def _():
            along(q, t, off, True, own).start()

        @pl.when(to_left(t))
        def _():
            along(q, t, off, False, own).start()

    def launch(t, _):
        for off in range(1, count):
            first(t, off).start()
        return 0

    both(0, 0, True)
    lax.fori_loop(0, chunks, launch, 0)
    hids = []
    for n, (a, b, e, dj) in enumerate(peers):
        hids.append(pltpu.make_async_remote_copy(
            src_ref=hidden_ref, dst_ref=hid_ref.at[dj, d * cols + c], send_sem=hid_send.at[n], recv_sem=hid_recv.at[n],
            device_id=(a, b, e), device_id_type=MESH,
        ))
        hids[-1].start()
    pj = lax.rem(j + 1, GROUP)
    cut = kept * CHUNK
    tail = pl.ds(cut, other_ref.shape[0] - cut)

    def teach(n, part):
        return pltpu.make_async_remote_copy(
            src_ref=teacher_ref.at[pj, part], dst_ref=other_ref.at[part], send_sem=teach_send.at[n], recv_sem=teach_recv.at[n],
            device_id=(q * GROUP + pj, c, d), device_id_type=MESH,
        )

    teaches = [teach(0, tail), teach(1, pl.ds(0, cut))]
    for copy in teaches:
        copy.start()

    def extra(n):
        return pltpu.make_async_remote_copy(
            src_ref=teacher_ref.at[j, tail] if n == 0 else other_ref.at[tail], dst_ref=extra_ref.at[n],
            send_sem=extra_send.at[n], recv_sem=extra_recv.at[n], device_id=(r + inward, c, d), device_id_type=MESH,
        )

    far = [pltpu.make_async_remote_copy(
        src_ref=hidden_ref, dst_ref=hid_ref.at[GROUP, d * cols + c], send_sem=far_send.at[0], recv_sem=far_recv.at[0],
        device_id=(r + inward, c, d), device_id_type=MESH,
    )]
    for n, (a, b, e, dj) in enumerate(peers):
        far.append(pltpu.make_async_remote_copy(
            src_ref=hid_ref.at[GROUP, d * cols + c], dst_ref=hid_ref.at[GROUP + dj, d * cols + c],
            send_sem=far_send.at[n + 1], recv_sem=far_recv.at[n + 1], device_id=(a, b, e), device_id_type=MESH,
        ))

    @pl.when(end)
    def _():
        far[0].start()

    own = pltpu.make_async_copy(pieces_ref.at[me], full_ref.at[slot(q, me)], own_sem.at[0])
    own.start()
    own_hid = pltpu.make_async_copy(hidden_ref, hid_ref.at[0, d * cols + c], own_sem.at[1])
    own_hid.start()

    def start_line(t, _):
        @pl.when(t > 0)
        def _():
            both(t, 0, True)

        for off in range(1, count):
            first(t, off).wait_recv()
            both(t, off)
        return 0

    lax.fori_loop(0, chunks, start_line, 0)

    @pl.when(end)
    def _():
        extra(0).start()
        teaches[0].wait_recv()
        extra(1).start()

    @pl.when(server)
    def _():
        far[0].wait_recv()
        for copy in far[1:]:
            copy.start()

    def step(k, _):
        def chunk(t, _):
            wanted = (t < kept) | ~end
            for off in range(count):
                @pl.when((q - k >= 0) & wanted)
                def _():
                    along(q - k, t, off, True).wait_recv()

                    @pl.when(to_right(t))
                    def _():
                        along(q - k, t, off, True).start()

                @pl.when((q + k < steps) & wanted)
                def _():
                    along(q + k, t, off, False).wait_recv()

                    @pl.when(to_left(t))
                    def _():
                        along(q + k, t, off, False).start()

            return 0

        return lax.fori_loop(0, chunks, chunk, 0)

    lax.fori_loop(1, steps, step, 0)

    def settle(block, _):
        def chunk(t, _):
            for off in range(count):
                @pl.when((block <= q) & to_right(t))
                def _():
                    along(block, t, off, True).wait_send()

                @pl.when((block >= q) & to_left(t))
                def _():
                    along(block, t, off, False).wait_send()

            return 0

        return lax.fori_loop(0, chunks, chunk, 0)

    lax.fori_loop(0, steps, settle, 0)

    def settle_first(t, _):
        for off in range(1, count):
            first(t, off).wait_send()
        return 0

    lax.fori_loop(0, chunks, settle_first, 0)
    for copy in hids:
        copy.wait()
    teaches[1].wait()
    teaches[0].wait_send()
    own.wait()
    own_hid.wait()

    @pl.when(end)
    def _():
        far[0].wait_send()
        extra(0).wait_send()
        extra(1).wait_send()

    @pl.when(~end)
    def _():
        teaches[0].wait_recv()

    @pl.when(server)
    def _():
        extra(0).wait_recv()
        extra(1).wait_recv()
        for copy in far[1:]:
            copy.wait()


def gather(rows, cols, depths, pieces, teacher, hidden):
    count, narrow, padded = pieces.shape
    width = teacher.shape[1]
    steps = rows // GROUP
    chunks = padded // CHUNK
    features, tokens = hidden.shape
    peers = GROUP * cols * depths - 1
    dma = pltpu.SemaphoreType.DMA
    any_space = pl.BlockSpec(memory_space=pl.ANY)
    line = (steps, chunks, count)
    return pl.pallas_call(
        functools.partial(gather_kernel, rows, cols, depths),
        out_shape=(
            jax.ShapeDtypeStruct((depths * rows, narrow, padded), pieces.dtype),
            jax.ShapeDtypeStruct((width, tokens), teacher.dtype),
            jax.ShapeDtypeStruct((GROUP, width - (chunks - SKIP) * CHUNK, tokens), teacher.dtype),
            jax.ShapeDtypeStruct((2 * GROUP, depths * cols, features, tokens), hidden.dtype),
        ),
        in_specs=[any_space] * 3,
        out_specs=[any_space] * 4,
        scratch_shapes=[
            dma((2,)), dma((chunks, count)), dma((chunks, count)), dma((steps + 1, chunks, count)), dma(line),
            dma((2,)), dma((2,)), dma((2,)), dma((2,)), dma((peers,)), dma((peers,)), dma((peers + 1,)), dma((peers + 1,)),
        ],
        compiler_params=pltpu.CompilerParams(collective_id=0, has_side_effects=True),
        name="gather",
    )(pieces, teacher, hidden)


def add_terms(full_ref, teacher_refs, hid_ref, acc, start, size, offset=0, sets=range(GROUP)):
    rows = full_ref[:, :, pl.ds(start, size)].reshape(-1, size)
    for n, teacher_ref in zip(sets, teacher_refs):
        hidden = hid_ref[n].reshape(rows.shape[0], -1)
        tokens = hidden.shape[1]
        student = lax.dot_general(rows, hidden, (((0,), (0,)), ((), ())), preferred_element_type=jnp.float32)
        student = student.reshape(size // 8, 8, tokens)
        teacher = teacher_ref[pl.ds(start - offset, size), :].astype(jnp.float32).reshape(size // 8, 8, tokens)
        top = jnp.maximum(acc[n, 0], jnp.max(student, axis=0))
        acc[n, 1] = acc[n, 1] * jnp.exp(acc[n, 0] - top) + jnp.sum(jnp.exp(student - top[None]), axis=0)
        acc[n, 0] = top
        teacher_top = jnp.maximum(acc[n, 2], jnp.max(teacher, axis=0))
        fade = jnp.exp(acc[n, 2] - teacher_top)
        weights = jnp.exp(teacher - teacher_top[None])
        acc[n, 3] = acc[n, 3] * fade + jnp.sum(weights, axis=0)
        acc[n, 4] = acc[n, 4] * fade + jnp.sum(weights * student, axis=0)
        acc[n, 2] = teacher_top


def terms_kernel(flags, full_ref, own_ref, other_ref, extra_ref, hid_ref, out_ref, acc):
    width = other_ref.shape[0]
    cut = width - extra_ref.shape[1]
    for n in range(2 * GROUP):
        for k in range(5):
            acc[n, k] = jnp.full(acc.shape[2:], LOW if k in (0, 2) else 0.0, jnp.float32)
    main = (own_ref.at[0], other_ref)
    extra = tuple(extra_ref.at[n] for n in range(GROUP))

    def tiles(begin, stop, refs, offset, sets):
        whole = (stop - begin) // TILE

        def tile(i, _):
            start = pl.multiple_of(begin + i * TILE, 128)
            add_terms(full_ref, refs, hid_ref, acc, start, TILE, offset, sets)
            return 0

        lax.fori_loop(0, whole, tile, 0)
        if (stop - begin) % TILE:
            add_terms(full_ref, refs, hid_ref, acc, begin + whole * TILE, (stop - begin) % TILE, offset, sets)

    tiles(0, cut, main, 0, range(GROUP))

    @pl.when(flags[1] == 0)
    def _():
        tiles(cut, width, main, 0, range(GROUP))

    @pl.when(flags[2] == 1)
    def _():
        tiles(cut, width, extra, cut, range(GROUP, 2 * GROUP))

    for n in range(2 * GROUP):
        values = merge([acc[n, k] for k in range(5)])
        out_ref[n] = jnp.concatenate(values + [values[0]] * 3, axis=0)


def merge(parts):
    top, total, teacher_top, teacher_total, cross = parts
    peak = jnp.max(top, axis=0, keepdims=True)
    teacher_peak = jnp.max(teacher_top, axis=0, keepdims=True)
    scale = jnp.exp(teacher_top - teacher_peak)
    return [
        peak,
        jnp.sum(total * jnp.exp(top - peak), axis=0, keepdims=True),
        teacher_peak,
        jnp.sum(teacher_total * scale, axis=0, keepdims=True),
        jnp.sum(cross * scale, axis=0, keepdims=True),
    ]


def terms(flags, full, teacher, other, extra, hid):
    tokens = other.shape[1]
    return pl.pallas_call(
        terms_kernel,
        out_shape=jax.ShapeDtypeStruct((2 * GROUP, 8, tokens), jnp.float32),
        grid_spec=pltpu.PrefetchScalarGridSpec(
            num_scalar_prefetch=1,
            grid=(1,),
            in_specs=[
                pl.BlockSpec(full.shape, lambda i, f: (0, 0, 0)),
                pl.BlockSpec((1,) + other.shape, lambda i, f: (f[0], 0, 0)),
                pl.BlockSpec(other.shape, lambda i, f: (0, 0)),
                pl.BlockSpec(extra.shape, lambda i, f: (0, 0, 0)),
                pl.BlockSpec(hid.shape, lambda i, f: (0, 0, 0, 0)),
            ],
            out_specs=pl.BlockSpec((2 * GROUP, 8, tokens), lambda i, f: (0, 0, 0)),
            scratch_shapes=[pltpu.VMEM((2 * GROUP, 5, 8, tokens), jnp.float32)],
        ),
        compiler_params=pltpu.CompilerParams(vmem_limit_bytes=60 * 2**20),
        name="terms",
    )(flags, full, teacher, other, extra, hid)


def combine_kernel(rows, cols, depths, stats_ref, loss_ref, peak_ref, held, send_sem, recv_sem):
    r, c, d, q, j = place(rows, cols, depths)
    end, server, inward = ends(rows, q)
    peers = group_peers(rows, cols, depths)
    near = len(peers)
    group = [(r, c, d, 0)] + peers
    barrier = greet([(a, b, e) for a, b, e, _ in peers])

    @pl.when(end)
    def _():
        greet([(a + inward, b, e) for a, b, e, _ in group])

    @pl.when(server)
    def _():
        greet([(a - inward, b, e) for a, b, e, _ in group])

    pl.semaphore_wait(barrier, near + as_count(end | server) * len(group))

    def send(n, a, b, e, source):
        return pltpu.make_async_remote_copy(
            src_ref=stats_ref.at[source], dst_ref=held.at[n], send_sem=send_sem.at[n], recv_sem=recv_sem.at[n],
            device_id=(a, b, e), device_id_type=MESH,
        )

    copies = [send(n, a, b, e, dj) for n, (a, b, e, dj) in enumerate(peers)]
    far = [send(near + n, a - inward, b, e, GROUP + dj) for n, (a, b, e, dj) in enumerate(group)]

    @pl.when(server)
    def _():
        for copy in far:
            copy.start()

    for copy in copies:
        copy.start()

    @pl.when(~end)
    def _():
        for n in range(len(group)):
            for k in range(5):
                held[near + n, k] = jnp.full(held.shape[2:], LOW if k in (0, 2) else 0.0, jnp.float32)

    for copy in copies:
        copy.wait()

    @pl.when(server)
    def _():
        for copy in far:
            copy.wait_send()

    @pl.when(end)
    def _():
        for copy in far:
            copy.wait_recv()

    blocks = [stats_ref[0]] + [held[n] for n in range(near + len(group))]
    parts = [jnp.concatenate([block[k : k + 1] for block in blocks], axis=0) for k in range(5)]
    peak, total, _, teacher_total, cross = merge(parts)
    norm_log = jnp.log(total)
    loss_ref[...] = peak + norm_log - cross / teacher_total
    peak_ref[...] = -norm_log


def combine(rows, cols, depths, stats):
    tokens = stats.shape[2]
    slots = 2 * GROUP * cols * depths - 1
    vmem = pl.BlockSpec(memory_space=pltpu.VMEM)
    return pl.pallas_call(
        functools.partial(combine_kernel, rows, cols, depths),
        out_shape=(jax.ShapeDtypeStruct((1, tokens), jnp.float32),) * 2,
        in_specs=[vmem],
        out_specs=(vmem, vmem),
        scratch_shapes=[
            pltpu.VMEM((slots, 8, tokens), jnp.float32),
            pltpu.SemaphoreType.DMA((slots,)),
            pltpu.SemaphoreType.DMA((slots,)),
        ],
        compiler_params=pltpu.CompilerParams(collective_id=1, has_side_effects=True),
        name="combine",
    )(stats)


def on_device(rows, cols, depths, student_hidden, embedding, teacher_logits):
    vocab, narrow = embedding.shape
    width = vocab // (depths * GROUP)
    pieces = embedding.T.reshape(narrow, depths * GROUP, width).transpose(1, 0, 2)
    pieces = jnp.pad(pieces, ((0, 0), (0, 0), (0, -width % CHUNK)))
    teacher = teacher_logits.T.reshape(GROUP, width, -1)
    full, other, extra, hid = gather(rows, cols, depths, pieces, teacher, student_hidden.T)
    row = lax.axis_index("row")
    end, server, _ = ends(rows, row // GROUP)
    flags = jnp.stack([lax.rem(row, GROUP), as_count(end), as_count(server)]).astype(jnp.int32)
    loss, peak = combine(rows, cols, depths, terms(flags, full, teacher, other, extra, hid))
    return loss.reshape(-1), peak.reshape(-1)


def solution(mesh):
    sizes = [mesh.shape[name] for name in ("row", "col", "depth")]
    in_specs = (P("row", ("depth", "col")), P("col", ("depth", "row")), P("row", ("col", "depth")))
    out_specs = (P("row"), P("row"))
    return jax.shard_map(
        functools.partial(on_device, *sizes), mesh=mesh, in_specs=in_specs, out_specs=out_specs, check_vma=False
    )
```
